32 devices in a mesh: mem: 4 (over x, core), col: 8 (over z, y).
Axes of the slice: x: 2, y: 2, z: 4, core: 2. Of those that a mesh axis runs over, the one named last changes fastest.
Arguments:
- prior: float32 [80, 2, 294912], P('mem', None, 'col'), may hold values from -15 to 15
- posterior: float32 [80, 2, 294912], P('mem', None, 'col'), may hold values from -8 to 8
- control: float32 [2, 294912], P(None, 'col'), may hold values from -4 to 4
- rtps_alpha: float32 [2], replicated, may hold values from 0.5 to 0.95
Outputs:
- analysis: float32 [80, 2, 294912], P('mem', None, 'col')
- spread_stats: float32 [4, 2], replicated
The draws below stay inside these ranges and needn't reach their ends.
All inputs are finite; a program needn't handle non-finite values.
Results may differ from the reference program's by a relative error of at most 0.0001.
Values sent between devices are 32-bit elements; how exact they have to be, the bound alone decides.
A program may use at most 64 MiB of HBM per device.

```python
import math
import jax
import jax.numpy as jnp
from jax import lax

LEV = 2
NLON = 1536
K = 80
NCOL = 294912
NLAT = 192


def column_scale(key, low, high):
    lat_rows = jnp.arange(NCOL, dtype=jnp.int32) // NLON
    place = (lat_rows.astype(jnp.float32) + 0.5) / NLAT
    smooth = low + (high - low) * jnp.sin(math.pi * place) ** 2
    rough = jnp.exp(jax.random.uniform(key, (LEV, NCOL), jnp.float32, -0.35, 0.35))
    return smooth[None, :] * rough


def ensemble(key, low, high):
    base = jnp.clip(jax.random.normal(jax.random.fold_in(key, 11), (LEV, NCOL), jnp.float32), -3.0, 3.0)
    scale = column_scale(jax.random.fold_in(key, 12), low, high)
    noise = jnp.clip(jax.random.normal(jax.random.fold_in(key, 13), (K, LEV, NCOL), jnp.float32), -4.0, 4.0)
    return base[None] + scale[None] * noise


def draw_prior(key, part):
    return ensemble(jax.random.fold_in(key, 101), 0.5, 2.0).astype(jnp.float32)


def draw_posterior(key, part):
    return ensemble(jax.random.fold_in(key, 202), 0.2, 0.8).astype(jnp.float32)


def steps_of(key, extent, pieces, smallest, largest):
    level, own = 1.0, jax.random.fold_in(key, 6)
    for position, blocks in pieces:
        heights = jnp.exp(jax.random.uniform(jax.random.fold_in(own, position), (blocks,), jnp.float32, smallest / len(pieces), largest / len(pieces)))
        level = level * jnp.repeat(heights, extent[position] // blocks).reshape([-1 if axis == position else 1 for axis in range(len(extent))])
    return level


def scatter_about(key, extent, spread, bound, split=(), kind=jnp.bfloat16):
    entries = jax.random.normal(key, extent, jnp.float32) * spread
    if len(split) > 0:
        entries = steps_of(key, extent, split, -0.22, 0.18) * entries
    return jnp.clip(entries, min=-bound, max=bound).astype(kind)


def setup_inputs(seed: int = 0) -> dict:
    key_of = jax.random.split(jax.random.key(seed), 5)
    return {
        "prior": draw_prior(jax.random.fold_in(key_of[4], 71), 0),
        "posterior": draw_posterior(jax.random.fold_in(key_of[4], 71), 0),
        "control": scatter_about(key_of[2], (LEV, NCOL), 1.0, 4.0, ((1, 8),), jnp.float32),
        "rtps_alpha": jnp.clip(jax.random.uniform(key_of[3], (LEV,), jnp.float32, 0.5, 0.95), 0.5, 0.95),
    }


spread_floor = 0.04

def area_weights():
    lat_rows = jnp.arange(NCOL, dtype=jnp.int32) // NLON
    latitude = (lat_rows.astype(jnp.float32) + 0.5) * (math.pi / NLAT) - math.pi / 2
    every_row = (jnp.arange(NLAT, dtype=jnp.int32).astype(jnp.float32) + 0.5) * (math.pi / NLAT) - math.pi / 2
    return (jnp.cos(latitude), NLON * jnp.sum(jnp.cos(every_row)))

def reference(prior, posterior, control, rtps_alpha):
    weight, weight_sum = area_weights()
    levels = []
    stat_rows = []
    for level in range(LEV):
        prior_level = prior[:, level, :]
        post_level = posterior[:, level, :]
        mean_b = lax.optimization_barrier(jnp.sum(prior_level, 0)) / K
        mean_a = lax.optimization_barrier(jnp.sum(post_level, 0)) / K
        var_b = lax.optimization_barrier(jnp.sum((prior_level - mean_b) ** 2, 0)) / (K - 1)
        var_a = lax.optimization_barrier(jnp.sum((post_level - mean_a) ** 2, 0)) / (K - 1)
        spread_b = jnp.sqrt(var_b)
        spread_raw = jnp.sqrt(var_a)
        spread_a = jnp.sqrt(var_a + spread_floor)
        relax = rtps_alpha[level]
        factor = (relax * spread_b + (1.0 - relax) * spread_a) / spread_a
        levels.append(control[level] + factor * (post_level - mean_a))
        shift_field = control[level] - mean_a
        stat_rows.append(jnp.stack([jnp.sum(weight * spread_b) / weight_sum, jnp.sum(weight * spread_raw) / weight_sum, jnp.sum(weight * factor * spread_raw) / weight_sum, jnp.sqrt(jnp.sum(weight * shift_field * shift_field) / weight_sum)]))
    analysis = jnp.stack(levels, axis=1)
    spread_stats = jnp.stack(stat_rows, axis=1)
    return (analysis, spread_stats)
```

```python
import functools
import math

import jax
import jax.numpy as jnp
from jax import lax
from jax.experimental import pallas as pl
from jax.experimental.pallas import tpu as pltpu
from jax.sharding import PartitionSpec as P

NLON = 1536
LANES = 128
PARTS = 3
AHEAD = 4

spread_floor = 0.04


def kernel(
    sizes,
    alpha_hbm,
    prior_hbm,
    post_hbm,
    control_hbm,
    out_ref,
    stats_ref,
    prior_v,
    control_v,
    send_a,
    recv_a,
    sum_x,
    recv_x,
    sum_own,
    field,
    slots,
    weight_v,
    alpha_ref,
    alpha_sem,
    load_sem,
    control_sem,
    a_send,
    a_recv,
    x_send,
    x_recv,
    r_send,
    r_recv,
    d_send,
    d_recv,
    t_send,
    t_recv,
    token,
):
    groups, tiles_n, col_tiles, lat_tiles, lat_count, weight_sum = sizes
    count, rows, _ = prior_v.shape
    members = count * groups
    quarter = rows // 4
    piece = quarter // PARTS
    me = lax.axis_index("mem")
    tile = lax.axis_index("col")
    core = lax.rem(me, 2)
    chip = lax.div(me, 2)
    other_core = chip * 2 + (1 - core)
    other_chip = (1 - chip) * 2 + core
    own = core * 2 + chip
    mine_far = core * 2 + (1 - chip)
    pair_far = (1 - core) * 2 + (1 - chip)
    pair_near = (1 - core) * 2 + chip

    def start(q, s):
        return pl.multiple_of(q * quarter + s * piece, 8)

    order = []
    for far, near in ((pair_far, mine_far), (pair_near, own)):
        for s in range(PARTS):
            order += [(far, s), (near, s)]
    loads = []
    for i, (q, s) in enumerate(order):
        span = pl.ds(start(q, s), piece)
        pair = []
        for k, (src, dst) in enumerate(((prior_hbm, prior_v), (post_hbm, out_ref))):
            copy = pltpu.make_async_copy(src.at[:, span, :], dst.at[:, span, :], load_sem.at[k, i])
            if i < AHEAD:
                copy.start()
            pair.append(copy)
        loads.append(pair)
    control_copy = pltpu.make_async_copy(
        control_hbm.at[pl.ds(pl.multiple_of(own * quarter, 8), quarter), :], control_v, control_sem
    )
    control_copy.start()
    alpha_copy = pltpu.make_async_copy(alpha_hbm, alpha_ref, alpha_sem)
    alpha_copy.start()

    barrier = pltpu.get_barrier_semaphore()
    others = [(a, d) for a in range(groups) for d in range(tiles_n) if (a, d) != (0, 0)]
    others.sort(key=sum, reverse=True)
    others = [{"mem": lax.rem(me + a, groups), "col": lax.rem(tile + d, tiles_n)} for a, d in others]
    cube = [{"mem": other_core}, {"mem": other_chip}]
    step = 1
    while step < tiles_n:
        cube.append({"col": tile + step - 2 * step * lax.rem(lax.div(tile, step), 2)})
        step *= 2
    for peer in cube:
        pl.semaphore_signal(barrier, inc=1, device_id=peer)
    rounds = len(cube)
    passed = [0]

    def tell():
        k = passed[0]
        if 0 < k < rounds:
            pl.semaphore_wait(token.at[k - 1], 1)
        if k + 1 < rounds:
            pl.semaphore_signal(token.at[k], inc=1, device_id=cube[k + 1])
        passed[0] = k + 1

    def send(src, dst, out_sem, in_sem, peer):
        return pltpu.make_async_remote_copy(
            src_ref=src, dst_ref=dst, send_sem=out_sem, recv_sem=in_sem, device_id=peer
        )

    started = []

    def sums(i, dst):
        q, s = order[i]
        span = pl.ds(start(q, s), piece)
        for k, ref in enumerate((prior_v, out_ref)):
            loads[i][k].wait()
            total = ref[0, span, :]
            square = total * total
            for m in range(1, count):
                v = ref[m, span, :]
                total = total + v
                square = square + v * v
            dst[2 * k] = total
            dst[2 * k + 1] = square
            if i + AHEAD < len(order):
                loads[i + AHEAD][k].start()

    a_copies = {}

    def to_pair(k, s):
        sums(k * 2 * PARTS + 2 * s, send_a.at[k, s])
        if (k, s) == (0, 0):
            pl.semaphore_wait(barrier, len(cube))
        copy = send(
            send_a.at[k, s], recv_a.at[k, s], a_send.at[k, s], a_recv.at[k, s], {"mem": other_core}
        )
        copy.start()
        a_copies[k, s] = copy
        started.append(copy)

    x_copies = {}

    def to_chip(s):
        a_copies[0, s].wait_recv()
        sum_x[s] = sum_x[s] + recv_a[0, s]
        copy = send(sum_x.at[s], recv_x.at[s], x_send.at[s], x_recv.at[s], {"mem": other_chip})
        copy.start()
        x_copies[s] = copy
        started.append(copy)

    for s in range(PARTS):
        to_pair(0, s)
        sums(2 * s + 1, sum_x.at[s])
        if s >= 1:
            to_chip(s - 1)
            if s in (1, PARTS - 1):
                tell()
    for s in range(PARTS):
        to_pair(1, s)
        if s == 0:
            to_chip(PARTS - 1)
        sums(2 * PARTS + 2 * s + 1, sum_own.at[s])
        if s in (PARTS // 2, PARTS - 1):
            tell()

    row = lax.broadcasted_iota(jnp.int32, (quarter, LANES), 0) + start(own, 0)
    place = lax.shift_right_logical(row, 1) + tile * col_tiles
    lat_row = jnp.floor((place.astype(jnp.float32) + 0.5) * (1.0 / lat_tiles))
    weight_v[...] = jnp.cos((lat_row + 0.5) * (math.pi / lat_count) - math.pi / 2)
    alpha_copy.wait()
    level = lax.rem(lax.broadcasted_iota(jnp.int32, (piece, LANES), 0), 2)
    relax = jnp.where(level == 0, alpha_ref[0], alpha_ref[1])
    control_copy.wait()
    acc = [jnp.zeros((8, LANES), jnp.float32) for _ in range(4)]
    r_copies, d_copies = {}, {}
    for s in range(PARTS):
        a_copies[1, s].wait_recv()
        near = sum_own[s] + recv_a[1, s]
        x_copies[s].wait_recv()
        total = near + recv_x[s]
        mean_b = total[0] / members
        mean_a = total[2] / members
        var_b = jnp.maximum(total[1] - total[0] * mean_b, 0.0) / (members - 1)
        var_a = jnp.maximum(total[3] - total[2] * mean_a, 0.0) / (members - 1)
        spread_b = jnp.sqrt(var_b)
        spread_raw = jnp.sqrt(var_a)
        spread_a = jnp.sqrt(var_a + spread_floor)
        factor = (relax * spread_b + (1.0 - relax) * spread_a) / spread_a
        control = control_v[pl.ds(s * piece, piece), :]
        field[own, s, 0] = factor
        field[own, s, 1] = control - factor * mean_a
        r_copies[s] = send(
            field.at[own, s], field.at[own, s], r_send.at[s], r_recv.at[s], {"mem": other_chip}
        )
        d_copies[0, s] = send(
            field.at[own, s], field.at[own, s], d_send.at[0, s], d_recv.at[0, s], {"mem": other_core}
        )
        r_copies[s].start()
        d_copies[0, s].start()
        started += [r_copies[s], d_copies[0, s]]
        if s < PARTS - 1:
            tell()
        weight = weight_v[pl.ds(s * piece, piece), :]
        shift = control - mean_a
        terms = (weight * spread_b, weight * spread_raw, weight * factor * spread_raw, weight * shift * shift)
        for k, term in enumerate(terms):
            for i in range(piece // 8):
                acc[k] = acc[k] + term[8 * i : 8 * i + 8]

    sub = lax.broadcasted_iota(jnp.int32, (8, LANES), 0)
    lane = lax.broadcasted_iota(jnp.int32, (8, LANES), 1)
    tile_sum = jnp.zeros((8, LANES), jnp.float32)
    for k in range(4):
        v = acc[k] + pltpu.roll(acc[k], 4, 0)
        v = v + pltpu.roll(v, 2, 0)
        tile_sum = jnp.where(lax.div(sub, 2) == k, v, tile_sum)
    tile_sum = jnp.broadcast_to(jnp.sum(tile_sum, 1, keepdims=True), (8, LANES))
    tile_sum = jnp.where(lane == lax.div(sub, 2), tile_sum, 0.0)
    tile_sum = tile_sum + pltpu.roll(tile_sum, 4, 0)
    tile_sum = tile_sum + pltpu.roll(tile_sum, 2, 0)
    while passed[0] < rounds:
        tell()
    here = slots.at[me * tiles_n + tile]
    here[...] = tile_sum[:2]
    t_copies = []
    for i, peer in enumerate(others):
        copy = send(here, here, t_send.at[i], t_recv.at[i], peer)
        copy.start()
        t_copies.append(copy)
        started.append(copy)

    def apply(q, s):
        span = pl.ds(start(q, s), piece)
        factor = field[q, s, 0]
        offset = field[q, s, 1]
        for m in range(count):
            out_ref[m, span, :] = out_ref[m, span, :] * factor + offset

    for s in range(PARTS):
        apply(own, s)

    for s in range(PARTS):
        r_copies[s].wait_recv()
        d_copies[1, s] = send(
            field.at[mine_far, s], field.at[mine_far, s], d_send.at[1, s], d_recv.at[1, s], {"mem": other_core}
        )
        d_copies[1, s].start()
        started.append(d_copies[1, s])
        d_copies[0, s].wait_recv()
        apply(pair_near, s)
        apply(mine_far, s)
        if s >= 1:
            d_copies[1, s - 1].wait_recv()
            apply(pair_far, s - 1)
    d_copies[1, PARTS - 1].wait_recv()
    apply(pair_far, PARTS - 1)

    for copy in t_copies:
        copy.wait_recv()
    whole = slots[0]
    for t in range(1, groups * tiles_n):
        whole = whole + slots[t]
    whole = whole / weight_sum
    whole = jnp.where(lane[:2] == 3, jnp.sqrt(whole), whole)
    stats_ref[...] = whole[:, :4]

    for copy in started:
        copy.wait_send()


def write_out(groups, analysis_v, stats_v, analysis_hbm, stats_hbm, write_sem, stats_sem):
    count = analysis_v.shape[0]
    copies = [pltpu.make_async_copy(stats_v, stats_hbm, stats_sem)]
    for g in range(groups):
        span = pl.ds(g * (count // groups), count // groups)
        copies.append(pltpu.make_async_copy(analysis_v.at[span], analysis_hbm.at[span], write_sem.at[g]))
    for copy in copies[1:] + copies[:1]:
        copy.start()
    for copy in copies:
        copy.wait()


def to_tiles(array):
    lead, (levels, columns) = array.shape[:-2], array.shape[-2:]
    split = array.reshape(*lead, levels, columns // LANES, LANES)
    return jnp.swapaxes(split, -3, -2).reshape(*lead, levels * columns // LANES, LANES)


def from_tiles(array, levels):
    lead, rows = array.shape[:-2], array.shape[-2]
    split = array.reshape(*lead, rows // levels, levels, LANES)
    return jnp.swapaxes(split, -3, -2).reshape(*lead, levels, rows // levels * LANES)


def local(groups, tiles_n, prior, posterior, control, rtps_alpha):
    count, levels, columns = prior.shape
    rows = levels * columns // LANES
    piece = rows // 4 // PARTS
    lat_count = columns * tiles_n // NLON
    weight_sum = NLON * math.fsum(
        math.cos((r + 0.5) * math.pi / lat_count - math.pi / 2) for r in range(lat_count)
    )
    sizes = (groups, tiles_n, columns // LANES, NLON // LANES, lat_count, weight_sum)
    f32 = jnp.float32
    dma = pltpu.SemaphoreType.DMA
    hbm = pl.BlockSpec(memory_space=pl.ANY)
    analysis, stats = pl.pallas_call(
        functools.partial(kernel, sizes),
        out_shape=(
            pltpu.VMEM((count, rows, LANES), f32),
            pltpu.VMEM((levels, 4), f32),
        ),
        in_specs=[hbm, hbm, hbm, hbm],
        out_specs=(pl.BlockSpec(memory_space=pltpu.VMEM), pl.BlockSpec(memory_space=pltpu.VMEM)),
        scratch_shapes=[
            pltpu.VMEM((count, rows, LANES), f32),
            pltpu.VMEM((rows // 4, LANES), f32),
            pltpu.VMEM((2, PARTS, 4, piece, LANES), f32),
            pltpu.VMEM((2, PARTS, 4, piece, LANES), f32),
            pltpu.VMEM((PARTS, 4, piece, LANES), f32),
            pltpu.VMEM((PARTS, 4, piece, LANES), f32),
            pltpu.VMEM((PARTS, 4, piece, LANES), f32),
            pltpu.VMEM((4, PARTS, 2, piece, LANES), f32),
            pltpu.VMEM((groups * tiles_n, levels, LANES), f32),
            pltpu.VMEM((rows // 4, LANES), f32),
            pltpu.SMEM((levels,), f32),
            dma,
            dma((2, 4 * PARTS)),
            dma,
            dma((2, PARTS)),
            dma((2, PARTS)),
            dma((PARTS,)),
            dma((PARTS,)),
            dma((PARTS,)),
            dma((PARTS,)),
            dma((2, PARTS)),
            dma((2, PARTS)),
            dma((groups * tiles_n - 1,)),
            dma((groups * tiles_n - 1,)),
            pltpu.SemaphoreType.REGULAR((2 + tiles_n.bit_length(),)),
        ],
        compiler_params=pltpu.CompilerParams(collective_id=0, has_side_effects=True, vmem_limit_bytes=56 * 1024 * 1024),
    )(rtps_alpha, to_tiles(prior), to_tiles(posterior), to_tiles(control))
    vmem = pl.BlockSpec(memory_space=pltpu.VMEM)
    writes = math.gcd(count, 10)
    analysis, stats = pl.pallas_call(
        functools.partial(write_out, writes),
        out_shape=(
            jax.ShapeDtypeStruct((count, rows, LANES), f32),
            jax.ShapeDtypeStruct((levels, 4), f32),
        ),
        in_specs=[vmem, vmem],
        out_specs=(hbm, hbm),
        scratch_shapes=[dma((writes,)), dma],
        compiler_params=pltpu.CompilerParams(vmem_limit_bytes=16 * 1024 * 1024),
    )(analysis, stats)
    return from_tiles(analysis, levels), stats.T


def solution(mesh):
    return jax.shard_map(
        functools.partial(local, mesh.shape["mem"], mesh.shape["col"]),
        mesh=mesh,
        in_specs=(P("mem", None, "col"), P("mem", None, "col"), P(None, "col"), P()),
        out_specs=(P("mem", None, "col"), P()),
        check_vma=False,
    )
```
